8 devices in a mesh: replica: 1 (over z), ep: 8 (over y, x, core).
Axes of the slice: x: 2, y: 2, z: 1, core: 2. Of those that a mesh axis runs over, the one named last changes fastest.
Arguments:
- hidden: bfloat16 [8192, 1536], P(('replica', 'ep'))
- route_one: int32 [8192, 8], P(('replica', 'ep'))
- gate_one: float32 [8192, 8], P(('replica', 'ep'))
- route_two: int32 [8192, 8], P(('replica', 'ep'))
- gate_two: float32 [8192, 8], P(('replica', 'ep'))
- w_gate_one: bfloat16 [64, 1536, 512], P('ep')
- w_up_one: bfloat16 [64, 1536, 512], P('ep')
- w_down_one: bfloat16 [64, 512, 1536], P('ep')
- w_gate_two: bfloat16 [64, 1536, 512], P('ep')
- w_up_two: bfloat16 [64, 1536, 512], P('ep')
- w_down_two: bfloat16 [64, 512, 1536], P('ep')
- old_map: int32 [2, 64], replicated
- new_map: int32 [2, 64], replicated
Outputs:
- output 1: bfloat16 [8192, 1536], P(('replica', 'ep'))
- output 2: bfloat16 [64, 1536, 512], P('ep')
- output 3: bfloat16 [64, 1536, 512], P('ep')
- output 4: bfloat16 [64, 512, 1536], P('ep')
- output 5: bfloat16 [64, 1536, 512], P('ep')
- output 6: bfloat16 [64, 1536, 512], P('ep')
- output 7: bfloat16 [64, 512, 1536], P('ep')
All inputs are finite; a program needn't handle non-finite values.
Results may differ from the reference program's by a relative error of at most 0.00519.
Values are sent between devices in bfloat16 or wider.
A program may use at most 1 GiB of HBM per device.

```python
import jax
import jax.numpy as jnp
from jax import lax

GROUP = 8
SLOTS = 8
TOK_DEV = 1024
D_MODEL = 1536
D_FF = 512
EXPERTS = 40
TOP = 8
ROW_BLOCK = 64

TOKENS = GROUP * TOK_DEV
NSLOTS = GROUP * SLOTS
ROWS = TOKENS * TOP
NBLOCKS = ROWS // ROW_BLOCK + EXPERTS + 1
HOT_COUNT = TOK_DEV // 2


def draw_layout(key):
    key_rot, key_lab, key_loc = jax.random.split(key, 3)
    slot_pos = jnp.arange(NSLOTS)
    dest_start = (GROUP // 2) * SLOTS
    in_dest = (slot_pos >= dest_start) & (slot_pos < dest_start + SLOTS)
    slot_rank = jnp.where(slot_pos < dest_start, slot_pos,
                          jnp.where(in_dest, NSLOTS - SLOTS + slot_pos - dest_start, slot_pos - SLOTS))
    old_base = jnp.where(slot_rank < EXPERTS, slot_rank,
                         EXPERTS - 1 - (slot_rank - EXPERTS) % (EXPERTS - SLOTS))
    new_base = jnp.where(in_dest, (slot_pos - dest_start) % SLOTS, old_base)
    local_perm = jax.random.permutation(key_loc, jnp.tile(jnp.arange(SLOTS), (GROUP, 1)), axis=1, independent=True)
    rot_shift = jax.random.randint(key_rot, (), 0, GROUP)
    dev_source = (jnp.arange(GROUP) - rot_shift) % GROUP
    relabel = jax.random.permutation(key_lab, EXPERTS)

    def place_layout(base_map):
        slot_grid = jnp.take_along_axis(base_map.reshape(GROUP, SLOTS), local_perm, axis=1)
        return relabel[slot_grid[dev_source]].reshape(NSLOTS).astype(jnp.int32)

    return place_layout(old_base), place_layout(new_base)


def draw_routes(key):
    key_exp, key_tok, key_col = jax.random.split(key, 3)
    rest_count = TOK_DEV * TOP - HOT_COUNT
    rank_ids = jnp.arange(EXPERTS)
    counts = jnp.where(rank_ids == 0, HOT_COUNT,
                       rest_count // (EXPERTS - 1) + (rank_ids - 1 < rest_count % (EXPERTS - 1)))
    run_end = jnp.cumsum(counts)
    run_of_pos = jnp.searchsorted(run_end, jnp.arange(TOK_DEV * TOP), side='right')
    exp_order = jax.random.permutation(key_exp, jnp.tile(jnp.arange(EXPERTS), (GROUP, 1)), axis=1, independent=True)
    listed = exp_order[:, run_of_pos]
    choices = listed.reshape(GROUP, TOP, TOK_DEV).transpose(0, 2, 1)
    tok_perm = jax.random.permutation(key_tok, jnp.tile(jnp.arange(TOK_DEV), (GROUP, 1)), axis=1, independent=True)
    choices = jnp.take_along_axis(choices, tok_perm[:, :, None], axis=1).reshape(TOKENS, TOP)
    return jax.random.permutation(key_col, choices, axis=1, independent=True).astype(jnp.int32)


def draw_weights(key, slot_map):
    key_gate, key_up, key_down = jax.random.split(key, 3)
    w_gate = jax.random.normal(key_gate, (EXPERTS, D_MODEL, D_FF), jnp.float32) * D_MODEL ** -0.5
    w_up = jax.random.normal(key_up, (EXPERTS, D_MODEL, D_FF), jnp.float32) * D_MODEL ** -0.5
    w_down = jax.random.normal(key_down, (EXPERTS, D_FF, D_MODEL), jnp.float32) * (1.5 * D_FF ** -0.5)
    return (w_gate[slot_map].astype(jnp.bfloat16), w_up[slot_map].astype(jnp.bfloat16),
            w_down[slot_map].astype(jnp.bfloat16))


def setup_inputs(seed: int = 0, part: int = 0) -> dict:
    root_key = jax.random.key(seed)
    shared_key, part_root = jax.random.split(root_key)
    part_keys = jax.random.split(jax.random.fold_in(part_root, part), 5)
    shared_keys = jax.random.split(shared_key, 4)
    old_one, new_one = draw_layout(shared_keys[0])
    old_two, new_two = draw_layout(shared_keys[1])
    w_gate_one, w_up_one, w_down_one = draw_weights(shared_keys[2], old_one)
    w_gate_two, w_up_two, w_down_two = draw_weights(shared_keys[3], old_two)
    gate_scale = TOP ** -0.5
    return {
        'hidden': jax.random.normal(part_keys[0], (TOKENS, D_MODEL), jnp.float32).astype(jnp.bfloat16),
        'route_one': draw_routes(part_keys[1]),
        'gate_one': jax.random.uniform(part_keys[2], (TOKENS, TOP), jnp.float32, 0.5, 1.5) * gate_scale,
        'route_two': draw_routes(part_keys[3]),
        'gate_two': jax.random.uniform(part_keys[4], (TOKENS, TOP), jnp.float32, 0.5, 1.5) * gate_scale,
        'w_gate_one': w_gate_one,
        'w_up_one': w_up_one,
        'w_down_one': w_down_one,
        'w_gate_two': w_gate_two,
        'w_up_two': w_up_two,
        'w_down_two': w_down_two,
        'old_map': jnp.stack([old_one, old_two]),
        'new_map': jnp.stack([new_one, new_two]),
    }


def moe_layer(hidden, route, gates, w_gate, w_up, w_down, slot_map):
    first_slot = jnp.argmax(slot_map[None, :] == jnp.arange(EXPERTS)[:, None], axis=1)
    flat_exp = route.reshape(ROWS)
    sort_order = jnp.argsort(flat_exp, stable=True).astype(jnp.int32)
    counts = jnp.zeros((EXPERTS,), jnp.int32).at[flat_exp].add(1)
    padded = (counts + ROW_BLOCK - 1) // ROW_BLOCK * ROW_BLOCK
    pad_end = jnp.cumsum(padded)
    pad_start = pad_end - padded
    count_start = jnp.cumsum(counts) - counts
    sorted_exp = flat_exp[sort_order]
    dest_pos = pad_start[sorted_exp] + jnp.arange(ROWS) - count_start[sorted_exp]
    row_ids = jnp.full((NBLOCKS * ROW_BLOCK,), ROWS, jnp.int32).at[dest_pos].set(sort_order)
    block_exp = jnp.minimum(jnp.searchsorted(pad_end, jnp.arange(NBLOCKS) * ROW_BLOCK, side='right'), EXPERTS - 1)
    hidden_pad = jnp.concatenate([hidden, jnp.zeros((1, D_MODEL), jnp.bfloat16)], axis=0)
    gate_pad = jnp.concatenate([gates.reshape(ROWS), jnp.zeros((1,), jnp.float32)], axis=0)

    def one_block(mixed, block):
        block_rows, block_expert = block
        slot_index = first_slot[block_expert]
        token_rows = block_rows // TOP
        rows_in = hidden_pad[token_rows]
        gate_act = jnp.dot(rows_in, w_gate[slot_index], preferred_element_type=jnp.float32)
        up_act = jnp.dot(rows_in, w_up[slot_index], preferred_element_type=jnp.float32)
        inner = (jax.nn.silu(gate_act) * up_act).astype(jnp.bfloat16)
        expert_out = jnp.dot(inner, w_down[slot_index], preferred_element_type=jnp.float32).astype(jnp.bfloat16)
        weighted = expert_out.astype(jnp.float32) * gate_pad[block_rows][:, None]
        return mixed.at[token_rows].add(weighted), None

    mixed, unused = lax.scan(one_block, jnp.zeros((TOKENS + 1, D_MODEL), jnp.float32),
                             (row_ids.reshape(NBLOCKS, ROW_BLOCK), block_exp))
    return (hidden.astype(jnp.float32) + mixed[:TOKENS]).astype(jnp.bfloat16)


def migrate(weights, old_row, new_row):
    first_old = jnp.argmax(old_row[None, :] == new_row[:, None], axis=1)
    source_slot = jnp.where(old_row == new_row, jnp.arange(NSLOTS), first_old)
    return weights[source_slot]


def reference(hidden, route_one, gate_one, route_two, gate_two, w_gate_one, w_up_one, w_down_one,
              w_gate_two, w_up_two, w_down_two, old_map, new_map):
    hidden_mid = moe_layer(hidden, route_one, gate_one, w_gate_one, w_up_one, w_down_one, old_map[0])
    hidden_out = moe_layer(hidden_mid, route_two, gate_two, w_gate_two, w_up_two, w_down_two, old_map[1])
    return (hidden_out,
            migrate(w_gate_one, old_map[0], new_map[0]),
            migrate(w_up_one, old_map[0], new_map[0]),
            migrate(w_down_one, old_map[0], new_map[0]),
            migrate(w_gate_two, old_map[1], new_map[1]),
            migrate(w_up_two, old_map[1], new_map[1]),
            migrate(w_down_two, old_map[1], new_map[1]))
```

```python
import jax
import jax.numpy as jnp
from jax import lax
from jax.experimental import pallas as pl
from jax.experimental.pallas import tpu as pltpu
from jax.sharding import PartitionSpec as P

CHUNKS = 4
TOK_BLOCK = 1024
ROW_TILE = 512


def dense_kernel(active_ref, x_ref, gate_ref, wg_ref, wu_ref, wd_ref, out_ref):
    slot = pl.program_id(1)
    tile_dev = ROW_TILE // gate_ref.shape[1]

    @pl.when(slot == 0)
    def _():
        out_ref[...] = jnp.zeros_like(out_ref)

    @pl.when(active_ref[slot] != 0)
    def _():
        def tile(step, carry):
            rows = pl.ds(pl.multiple_of(step * ROW_TILE, ROW_TILE), ROW_TILE)
            x = x_ref[rows, :]
            gate_act = jnp.dot(x, wg_ref[0], preferred_element_type=jnp.float32)
            up_act = jnp.dot(x, wu_ref[0], preferred_element_type=jnp.float32)
            inner = (gate_act * jax.nn.sigmoid(gate_act) * up_act).astype(jnp.bfloat16)
            gates = gate_ref[pl.ds(step * tile_dev, tile_dev)].reshape(ROW_TILE, gate_ref.shape[2])
            lane = lax.broadcasted_iota(jnp.int32, gates.shape, 1)
            gate = jnp.sum(jnp.where(lane == slot, gates, 0.0), axis=1, keepdims=True)
            expert_out = jnp.dot(inner, wd_ref[0], preferred_element_type=jnp.float32)
            expert_out = expert_out.astype(jnp.bfloat16).astype(jnp.float32)
            out_ref[rows, :] += jnp.where(gate != 0.0, gate * expert_out, 0.0)
            return carry

        lax.fori_loop(0, x_ref.shape[0] // ROW_TILE, tile, 0)


def dense_experts(x, gates, chunk, active, w_gate, w_up, w_down):
    rows, d_model = x.shape
    slots, _, d_ff = w_gate.shape
    group, tok_dev, _ = gates.shape
    per_dev = rows // group
    block_dev = TOK_BLOCK // per_dev
    return pl.pallas_call(
        dense_kernel,
        out_shape=jax.ShapeDtypeStruct((rows, d_model), jnp.float32),
        grid_spec=pltpu.PrefetchScalarGridSpec(
            num_scalar_prefetch=1,
            grid=(rows // TOK_BLOCK, slots),
            in_specs=[
                pl.BlockSpec((TOK_BLOCK, d_model), lambda t, s, a: (t, 0)),
                pl.BlockSpec((block_dev, per_dev, slots), lambda t, s, a: (t, chunk, 0)),
                pl.BlockSpec((1, d_model, d_ff), lambda t, s, a: (s, 0, 0)),
                pl.BlockSpec((1, d_model, d_ff), lambda t, s, a: (s, 0, 0)),
                pl.BlockSpec((1, d_ff, d_model), lambda t, s, a: (s, 0, 0)),
            ],
            out_specs=pl.BlockSpec((TOK_BLOCK, d_model), lambda t, s, a: (t, 0)),
        ),
        compiler_params=pltpu.CompilerParams(
            dimension_semantics=('arbitrary', 'arbitrary'), vmem_limit_bytes=60 * 1024 * 1024),
        cost_estimate=pl.CostEstimate(
            flops=rows * slots * 6 * d_model * d_ff, transcendentals=rows * slots * d_ff,
            bytes_accessed=rows * d_model * 6 + (rows // TOK_BLOCK) * slots * 6 * d_model * d_ff),
        name='dense_experts',
    )(active, x, gates, w_gate, w_up, w_down)


def add_kernel(hidden_ref, mixed_ref, out_ref):
    out_ref[...] = (hidden_ref[...].astype(jnp.float32) + mixed_ref[...]).astype(out_ref.dtype)


def add_mixed(hidden, mixed):
    return pl.pallas_call(
        add_kernel,
        out_shape=jax.ShapeDtypeStruct(hidden.shape, hidden.dtype),
        cost_estimate=pl.CostEstimate(flops=2_000_000, transcendentals=0, bytes_accessed=hidden.size * 8),
        name='add_mixed',
    )(hidden, mixed)


def place_kernel(own_idx, in_idx, changed, *refs):
    own, incoming, outs = refs[0:3], refs[3:6], refs[6:9]
    slot = pl.program_id(0)

    @pl.when(changed[slot] != 0)
    def _():
        for src, dst in zip(incoming, outs):
            dst[...] = src[...]

    @pl.when(changed[slot] == 0)
    def _():
        for src, dst in zip(own, outs):
            dst[...] = src[...]


def place_layer(own, incoming, source, changed):
    slots = own[0].shape[0]
    own_idx = jnp.where(changed, 0, jnp.arange(slots)).astype(jnp.int32)
    in_idx = jnp.where(changed, source, 0).astype(jnp.int32)

    def block(weight):
        return (1,) + weight.shape[1:]

    return pl.pallas_call(
        place_kernel,
        out_shape=[jax.ShapeDtypeStruct(w.shape, w.dtype) for w in own],
        grid_spec=pltpu.PrefetchScalarGridSpec(
            num_scalar_prefetch=3,
            grid=(slots,),
            in_specs=[pl.BlockSpec(block(w), lambda s, o, i, c: (o[s], 0, 0)) for w in own]
            + [pl.BlockSpec(block(w), lambda s, o, i, c: (i[s], 0, 0)) for w in own],
            out_specs=[pl.BlockSpec(block(w), lambda s, o, i, c: (s, 0, 0)) for w in own],
        ),
        compiler_params=pltpu.CompilerParams(
            dimension_semantics=('arbitrary',), vmem_limit_bytes=60 * 1024 * 1024),
        cost_estimate=pl.CostEstimate(
            flops=30_000_000, transcendentals=0, bytes_accessed=2 * sum(w.size * 2 for w in own)),
        name='place_slots',
    )(own_idx, in_idx, changed.astype(jnp.int32), *own, *incoming)


def first_holder(row):
    same = row[:, None] == row[None, :]
    index = jnp.arange(row.shape[0])
    return ~jnp.any(same & (index[None, :] < index[:, None]), axis=1)


def solution(mesh):
    group = mesh.shape['ep']
    tok_spec = P(('replica', 'ep'), None)
    slot_spec = P('ep', None, None)
    map_spec = P(None, None)

    def body(hidden, route_one, gate_one, route_two, gate_two, w_gate_one, w_up_one, w_down_one,
             w_gate_two, w_up_two, w_down_two, old_map, new_map):
        device = lax.axis_index('ep')
        tok_dev, top = route_one.shape
        slots = w_gate_one.shape[0]
        per_chunk = tok_dev // CHUNKS
        weights = ((w_gate_one, w_up_one, w_down_one), (w_gate_two, w_up_two, w_down_two))

        def gather_chunk(rows):
            return lax.all_gather(rows, 'ep', axis=0, tiled=True)

        packed = jnp.concatenate(
            [route_one.T.astype(jnp.float32), gate_one.T, route_two.T.astype(jnp.float32), gate_two.T], axis=0)
        packed = lax.all_gather(packed, 'ep', axis=0, tiled=False)

        gates, actives, dests, placements = [], [], [], []
        for layer in range(2):
            old_row, new_row = old_map[layer], new_map[layer]
            mine = lax.dynamic_slice(old_row, (device * slots,), (slots,))
            active = lax.dynamic_slice(first_holder(old_row), (device * slots,), (slots,))
            route = packed[:, 2 * layer * top:(2 * layer + 1) * top, :]
            gate = packed[:, (2 * layer + 1) * top:(2 * layer + 2) * top, :]
            hit = (route[:, None] == mine.astype(jnp.float32)[None, :, None, None]) & active[None, :, None, None]
            local = jnp.sum(jnp.where(hit, gate[:, None], 0.0), axis=2)
            gates.append(local.transpose(0, 2, 1))
            actives.append(active.astype(jnp.int32))
            dests.append((jnp.argmax(old_row != new_row) // slots).astype(jnp.int32))
            from_dev = (device + group // 2) % group
            old_from = lax.dynamic_slice(old_row, (from_dev * slots,), (slots,))
            new_mine = lax.dynamic_slice(new_row, (device * slots,), (slots,))
            source = jnp.argmax(new_mine[:, None] == old_from[None, :], axis=1)
            placements.append((source, mine != new_mine))

        def compute(layer, chunk, rows):
            return dense_experts(rows, gates[layer], chunk, actives[layer], *weights[layer])

        def compute_and_send(layer, chunk, rows, weight):
            def branch(dest):
                def run(rows, weight):
                    pair = [((dest + group // 2) % group, dest)]
                    return compute(layer, chunk, rows), lax.ppermute(weight, 'ep', pair)
                return run
            return lax.switch(dests[layer], [branch(dest) for dest in range(group)], rows, weight)

        incoming = [[], []]
        states = [hidden[chunk * per_chunk:(chunk + 1) * per_chunk] for chunk in range(CHUNKS)]
        for layer in range(2):
            gathered = [gather_chunk(rows) for rows in states]
            for chunk in range(CHUNKS):
                if chunk < 3:
                    partial, moved = compute_and_send(layer, chunk, gathered[chunk], weights[layer][chunk])
                    incoming[layer].append(moved)
                else:
                    partial = compute(layer, chunk, gathered[chunk])
                mixed = lax.psum_scatter(partial, 'ep', scatter_dimension=0, tiled=True)
                states[chunk] = add_mixed(states[chunk], mixed)
        hidden_out = jnp.concatenate(states, axis=0)
        placed = [place_layer(weights[layer], incoming[layer], *placements[layer]) for layer in range(2)]
        return (hidden_out, *placed[0], *placed[1])

    in_specs = (tok_spec,) * 5 + (slot_spec,) * 6 + (map_spec, map_spec)
    out_specs = (tok_spec,) + (slot_spec,) * 6
    return jax.shard_map(body, mesh=mesh, in_specs=in_specs, out_specs=out_specs, check_vma=False)
```
